768 devices in a mesh: wave: 64 (over y, x, core), lev: 12 (over z).
Axes of the slice: x: 4, y: 8, z: 12, core: 2. Of those that a mesh axis runs over, the one named last changes fastest.
Arguments:
- spec: bfloat16 [128, 384, 640], P('wave', 'lev'), may hold values from -0.5 to 0.5
- legendre: bfloat16 [128, 1280, 640], P('wave'), may hold values from -0.25 to 0.25
- layer_depth_share: float32 [48], P('lev'), may hold values from 0.5 to 2
- quad_weight: float32 [1280], replicated, may hold values from 8 to 32
- wave_of_slot: int32 [128], P('wave'), may hold values from 0 to 639, as said below
Outputs:
- tendency: bfloat16 [128, 384, 640], P('wave', 'lev')
The draws below stay inside these ranges and needn't reach their ends.
Inputs may be any that keep to these rules, and one draw needn't show every extreme that they name: `wave_of_slot`: slots 2 i and 2 i + 1 hold wavenumbers m and 639 - m; no wavenumber appears twice.
All inputs are finite; a program needn't handle non-finite values.
Results may differ from the reference program's by a relative error of at most 0.0047.
The reference program's roundings to bfloat16 on the way count: a program that leaves them out, or rounds other values in their place, can miss the bound.
Values may be sent and summed in bfloat16 or wider, within the bound.
A program may use at most 128 MiB of HBM per device.

```python
import math
import jax
import jax.numpy as jnp
from jax import lax

LAT = 1280
ORDER_SPAN = 640
QUANTITY_TOTAL = 4
EASTWARD_MODES = 128
LEVELS = 48
COLS = 384
MAXLON = 2576
N_LEV = 12


def draw_wave_of_slot(key, part):
    chosen = jax.random.permutation(key, ORDER_SPAN // 2)[:EASTWARD_MODES // 2].astype(jnp.int32)
    return jnp.stack([chosen, ORDER_SPAN - 1 - chosen], axis=1).reshape(EASTWARD_MODES)


def level_of(own_key, shape, cuts, smallest, high):
    gain, own = 1.0, jax.random.fold_in(own_key, 6)
    for dim, parts in cuts:
        draws = jnp.exp(jax.random.uniform(jax.random.fold_in(own, dim), (parts,), jnp.float32, smallest / len(cuts), high / len(cuts)))
        gain = gain * jnp.repeat(draws, shape[dim] // parts).reshape([-1 if axis == dim else 1 for axis in range(len(shape))])
    return gain


def noise(key, shape, scale, reach, pieces=(), kind=jnp.bfloat16):
    level = level_of(key, shape, pieces, -0.22, 0.18) if pieces else 1.0
    values = jax.random.normal(key, shape, jnp.float32) * scale * level
    return jnp.minimum(jnp.maximum(values, -reach), reach).astype(kind)


def setup_inputs(seed: int = 0) -> dict:
    key_of = jax.random.split(jax.random.key(seed), 6)
    spec = noise(key_of[0], (EASTWARD_MODES, COLS, ORDER_SPAN), EASTWARD_MODES ** -0.5, 0.5, ((0, 64), (1, 12)))
    legendre = noise(key_of[1], (EASTWARD_MODES, LAT, ORDER_SPAN), ORDER_SPAN ** -0.5, 0.25, ((0, 64),))
    layer_depth_share = jnp.clip(jnp.exp(math.log(2.0) - 1.3862944 * jax.random.uniform(key_of[2], (LEVELS,), jnp.float32) ** level_of(key_of[2], (LEVELS,), ((0, 12),), -0.2, 0.2)), 0.5, 2.0)
    quad_weight = jnp.clip(jnp.exp(jax.random.uniform(key_of[3], (LAT,), jnp.float32, math.log(8.0), math.log(32.0))), 8.0, 32.0)
    wave_of_slot = draw_wave_of_slot(jax.random.fold_in(key_of[5], 71), 0)
    return {"spec": spec, "legendre": legendre, "layer_depth_share": layer_depth_share, "quad_weight": quad_weight, "wave_of_slot": wave_of_slot}


full_turn = 2.0 * math.pi


def rate_bundle(eastward_velocity, northward_velocity, local_curl_spin, thermal_state, planetary_rotation_effect, processor_dimension):
    absolute = local_curl_spin + planetary_rotation_effect
    return jnp.stack([absolute * eastward_velocity, absolute * northward_velocity,
                      0.5 * (eastward_velocity * eastward_velocity + northward_velocity * northward_velocity),
                      eastward_velocity * thermal_state], axis=processor_dimension)


def reference(spec, legendre, layer_depth_share, quad_weight, wave_of_slot):
    layers_on_processor = LEVELS // N_LEV
    degree_index = jnp.arange(ORDER_SPAN, dtype=jnp.int32)
    valid_cols = degree_index[None, :] < (ORDER_SPAN - wave_of_slot)[:, None]
    screened_entries = jnp.where(valid_cols[:, None, :], spec, jnp.zeros_like(spec))

    def inverse_one(inputs):
        leg_table, coeffs = inputs
        return jnp.dot(leg_table, coeffs.T, preferred_element_type=jnp.float32).astype(jnp.bfloat16)

    fourier = jnp.moveaxis(lax.map(inverse_one, (legendre, screened_entries)), 1, 0)
    points = jnp.arange(MAXLON, dtype=jnp.int32)
    weight_two = jnp.where(wave_of_slot == 0, 1.0, 2.0).astype(jnp.float32)

    def grid_one(inputs):
        latitude, coeffs = inputs
        length = 20 + 4 * jnp.minimum(latitude, LAT - 1 - latitude)
        length_f = length.astype(jnp.float32)
        phase_int = (wave_of_slot[:, None] * points[None, :]) % length
        angles = phase_int.astype(jnp.float32) * full_turn / length_f
        cosine = jnp.cos(angles)
        sine_vals = jnp.sin(angles)
        resolved = 2 * wave_of_slot < length
        amplitude = jnp.where(resolved, weight_two, 0.0)[:, None]
        split_parts = coeffs.reshape(EASTWARD_MODES, N_LEV, 2, QUANTITY_TOTAL, layers_on_processor)
        real_part = split_parts[:, :, 0].reshape(EASTWARD_MODES, -1)
        imag_part = split_parts[:, :, 1].reshape(EASTWARD_MODES, -1)
        grid_vals = jnp.dot(real_part.T, (amplitude * cosine).astype(jnp.bfloat16), preferred_element_type=jnp.float32)
        grid_vals = grid_vals - jnp.dot(imag_part.T, (amplitude * sine_vals).astype(jnp.bfloat16), preferred_element_type=jnp.float32)
        grid_vals = grid_vals.reshape(N_LEV, QUANTITY_TOTAL, layers_on_processor, MAXLON)
        planetary_rotation_effect = 2.0 * jnp.cos((latitude.astype(jnp.float32) + 0.5) * (math.pi / LAT))
        products = rate_bundle(grid_vals[:, 0], grid_vals[:, 1], grid_vals[:, 2], grid_vals[:, 3], planetary_rotation_effect, 1)
        products = products.astype(jnp.bfloat16).reshape(N_LEV * QUANTITY_TOTAL * layers_on_processor, MAXLON)
        live_mask = (points[None, :] < length) & resolved[:, None]
        cos_back = jnp.where(live_mask, cosine, 0.0).astype(jnp.bfloat16)
        sin_back = jnp.where(live_mask, sine_vals, 0.0).astype(jnp.bfloat16)
        row_scale = quad_weight[latitude] / length_f
        real_back = jnp.dot(products, cos_back.T, preferred_element_type=jnp.float32) * row_scale
        imag_back = -jnp.dot(products, sin_back.T, preferred_element_type=jnp.float32) * row_scale
        merged = jnp.stack([real_back.T.reshape(EASTWARD_MODES, N_LEV, QUANTITY_TOTAL, layers_on_processor),
                            imag_back.T.reshape(EASTWARD_MODES, N_LEV, QUANTITY_TOTAL, layers_on_processor)], axis=2)
        return merged.reshape(EASTWARD_MODES, COLS).astype(jnp.bfloat16)

    tend_rows = lax.map(grid_one, (jnp.arange(LAT, dtype=jnp.int32), fourier))

    def direct_one(inputs):
        leg_table, coeffs = inputs
        return jnp.dot(coeffs.T, leg_table, preferred_element_type=jnp.float32)

    tendency = lax.map(direct_one, (legendre, jnp.moveaxis(tend_rows, 1, 0)))
    thermal_state = screened_entries.reshape(EASTWARD_MODES, N_LEV, 2, QUANTITY_TOTAL, layers_on_processor, ORDER_SPAN)[:, :, :, 3].astype(jnp.float32)
    scaled_entries = thermal_state * layer_depth_share.reshape(N_LEV, 1, layers_on_processor, 1)
    scaled_entries = jnp.moveaxis(scaled_entries, 2, 1).reshape(EASTWARD_MODES, 2, LEVELS, ORDER_SPAN)
    below_sum = jnp.flip(jnp.cumsum(jnp.flip(scaled_entries, 2), 2), 2)
    geopot = jnp.moveaxis(below_sum.reshape(EASTWARD_MODES, 2, N_LEV, layers_on_processor, ORDER_SPAN), 1, 2)
    tendency = tendency.reshape(EASTWARD_MODES, N_LEV, 2, QUANTITY_TOTAL, layers_on_processor, ORDER_SPAN)
    tendency = tendency.at[:, :, :, 2].add(geopot)
    tendency = jnp.where(valid_cols[:, None, None, None, None, :], tendency, 0.0)
    return tendency.reshape(EASTWARD_MODES, COLS, ORDER_SPAN).astype(jnp.bfloat16)
```

```python
import functools
import math

import jax
import jax.numpy as jnp
from jax import lax
from jax.experimental import pallas as pl
from jax.experimental.pallas import tpu as pltpu
from jax.sharding import PartitionSpec as P

MESH = pl.DeviceIdType.MESH
F32 = jnp.float32
BF16 = jnp.bfloat16
ROWS = 16
LOW = 64
NT = (((1,), (1,)), ((), ()))


def round_up(x, step):
    return -(-x // step) * step


def iota(shape, dim):
    return lax.broadcasted_iota(jnp.int32, shape, dim)


def cos_sin(turns, quarter, length):
    count = jnp.floor(turns * (1.0 / quarter) + 0.5)
    x = (turns - count * quarter) * (2.0 * math.pi / length)
    y = x * x
    sine = x + x * y * (-1 / 6 + y * (1 / 120 + y * (-1 / 5040 + y * (1 / 362880))))
    cosine = 1.0 + y * (-0.5 + y * (1 / 24 + y * (-1 / 720 + y * (1 / 40320))))
    turn = count.astype(jnp.int32)
    swap = (turn & 1) == 1
    one = jnp.where(swap, sine, cosine)
    two = jnp.where(swap, cosine, sine)
    return jnp.where(((turn + 1) & 2) == 2, -one, one), jnp.where((turn & 2) == 2, -two, two)


class Plan:
    def __init__(self, mesh):
        self.groups = mesh.shape["wave"]
        self.depth = mesh.shape["lev"]
        self.lat = 1280
        self.span = 640
        self.quarter = self.lat // 4
        self.quads = self.quarter // self.groups
        self.blocks = []
        first = 0
        for quad in range(self.quads):
            low = quad * self.groups
            high = low + self.groups - 1
            for which in range(2):
                longest = 20 + 4 * (high if which == 0 else self.lat // 2 - 1 - low)
                points = round_up(longest, 128)
                self.blocks.append((quad, which, points, first))
                first += points
        self.table_rows = first
        self.coarse = round_up(max(b[2] for b in self.blocks) // LOW, 8)


def kernel(
    plan,
    spec_hbm, leg_hbm, share_hbm, quad_hbm, wave_hbm, out_ref,
    spec, leg, share, quad, waves,
    wave_row, wave_rows, stage, msg_out, msg_in, ret_out, ret_in,
    coefs, base, table, level_out, level_in, below,
    load_sem, wave_send, wave_recv, out_send, out_recv, ret_send, ret_recv, lev_send, lev_recv,
):
    n, depth, quads, span = plan.groups, plan.depth, plan.quads, plan.span
    me = lax.axis_index("wave")
    lev = lax.axis_index("lev")
    quarter = plan.quarter

    barrier = pltpu.get_barrier_semaphore()

    def greet(k, c):
        pl.semaphore_signal(barrier, inc=1, device_id={"wave": lax.rem(me + k, n)}, device_id_type=MESH)
        return c

    lax.fori_loop(1, n, greet, 0)

    def greet_level(k, c):
        pl.semaphore_signal(barrier, inc=1, device_id={"lev": k}, device_id_type=MESH)
        return c

    lax.fori_loop(lev + 1, depth, greet_level, 0)

    loads = [
        pltpu.make_async_copy(wave_hbm, waves, load_sem.at[0]),
        pltpu.make_async_copy(spec_hbm, spec, load_sem.at[1]),
        pltpu.make_async_copy(share_hbm, share, load_sem.at[2]),
        pltpu.make_async_copy(quad_hbm, quad, load_sem.at[3]),
        pltpu.make_async_copy(leg_hbm.at[0], leg.at[0], load_sem.at[4]),
        pltpu.make_async_copy(leg_hbm.at[1], leg.at[1], load_sem.at[5]),
    ]
    for load in loads:
        load.start()
    loads[0].wait()
    lane = iota((1, 128), 1)
    row = jnp.where(lane == me, waves[0], 0) + jnp.where(lane == me + n, waves[1], 0)
    wave_row[...] = row.astype(F32)
    loads[1].wait()
    loads[2].wait()

    column = iota((1, span), 1)
    masked = []
    for slot in range(2):
        live = column < span - waves[slot]
        values = jnp.where(live, spec[slot].astype(F32), 0.0)
        masked.append(values.astype(BF16))
        for part in range(2):
            total = jnp.zeros((1, span), F32)
            for l in (3, 2, 1, 0):
                at = part * 16 + 12 + l
                total = total + values[at : at + 1] * share[l]
                below[slot, part, l : l + 1, :] = total
            level_out[slot * 2 + part : slot * 2 + part + 1, :] = total

    where_row = iota((128, 32), 0)
    where_col = iota((128, 32), 1)
    column_of = (where_col // 16) * 64 + (where_col // 4 % 4) * 8 + where_col % 4
    place = []
    for k in range(4):
        which = 1 if k in (1, 2) else 0
        south = k // 2
        place.append((where_row == column_of + which * 32 + south * 4).astype(BF16))
    flip = (iota((n, n), 0) + iota((n, n), 1) == n - 1).astype(BF16)

    stage[...] = jnp.zeros_like(stage)
    for slot in range(2):
        loads[4 + slot].wait()
        sums = []
        for pair in ((0, 2), (1, 3)):
            acc = None
            for k in pair:
                weights = jnp.dot(place[k], masked[slot], preferred_element_type=F32).astype(BF16)
                term = lax.dot_general(
                    leg[slot, k * quarter : (k + 1) * quarter, :], weights, NT, preferred_element_type=F32
                )
                acc = term if acc is None else acc + term
            sums.append(acc)
        forward, backward = sums[0], sums[1].astype(BF16)
        for b in range(quads):
            other = quads - 1 - b
            turned = jnp.dot(flip, backward[other * n : (other + 1) * n], preferred_element_type=F32)
            stage[pl.ds(slot * quads + b, n, stride=ROWS), :] = forward[b * n : (b + 1) * n] + turned
    msg_out[...] = stage[...].astype(BF16).reshape(n, ROWS, 128)

    pl.semaphore_wait(barrier, n - 1 + lev)

    def send_wave(k, c):
        pltpu.make_async_remote_copy(
            wave_row, wave_rows.at[me], wave_send, wave_recv,
            device_id={"wave": lax.rem(me + k, n)}, device_id_type=MESH,
        ).start()
        return c

    lax.fori_loop(1, n, send_wave, 0)

    def send_out(k, c):
        to = lax.rem(me + k, n)
        pltpu.make_async_remote_copy(
            msg_out.at[to], msg_in.at[me], out_send, out_recv, device_id={"wave": to}, device_id_type=MESH
        ).start()
        return c

    lax.fori_loop(1, n, send_out, 0)

    def level_copy(source, to):
        return pltpu.make_async_remote_copy(
            level_out, level_in.at[source], lev_send.at[to], lev_recv.at[source],
            device_id={"lev": to}, device_id_type=MESH,
        )

    def send_level(k, c):
        level_copy(lev, k).start()
        return c

    lax.fori_loop(0, lev, send_level, 0)
    wave_rows[me] = wave_row[...]
    msg_in[me] = msg_out[me]
    others = pl.ds(0, n - 1)
    pltpu.make_async_copy(wave_rows.at[others], wave_rows.at[others], wave_recv).wait()
    m = jnp.sum(wave_rows[...], axis=0)

    loads[3].wait()
    rows = LOW + plan.coarse
    index = iota((rows, 1), 0)
    step = jnp.where(index < LOW, index, (index - LOW) * LOW).astype(F32)
    turns = step * m
    lengths = []
    for at, (b, which, points, first) in enumerate(plan.blocks):
        q = me + b * n
        if which == 1:
            q = plan.lat // 2 - 1 - q
        quart = (5 + q).astype(F32)
        lengths.append((q, quart * 4.0))
        c, s = cos_sin(turns, quart, quart * 4.0)
        base[at, 0] = c
        base[at, 1] = s

    for at, (b, which, points, first) in enumerate(plan.blocks):

        def expand(a, c, at=at, first=first):
            cl, sl = base[at, 0, pl.ds(0, LOW), :], base[at, 1, pl.ds(0, LOW), :]
            ch, sh = base[at, 0, pl.ds(LOW + a, 1), :], base[at, 1, pl.ds(LOW + a, 1), :]
            to = pl.ds(pl.multiple_of(first + a * LOW, LOW), LOW)
            table[to, 0:128] = (ch * cl - sh * sl).astype(BF16)
            table[to, 128:256] = (sh * cl + ch * sl).astype(BF16)
            return c

        lax.fori_loop(0, points // LOW, expand, 0)

    pltpu.make_async_copy(msg_in.at[others], msg_in.at[others], out_recv).wait()
    stage[...] = msg_in[...].reshape(n * ROWS, 128).astype(F32)
    double = jnp.where(m == 0.0, 1.0, 2.0)
    open_ = [2.0 * m < length for _, length in lengths]
    for b in range(quads):
        rows_in = [stage[pl.ds(slot * quads + b, n, stride=ROWS), :] for slot in range(2)]
        turned = jnp.concatenate(rows_in, axis=0).T
        for which in range(2):
            amplitude = jnp.where(open_[2 * b + which], double, 0.0)
            real = turned[which * 32 : which * 32 + 32] * amplitude
            imag = turned[64 + which * 32 : 96 + which * 32] * -amplitude
            coefs[2 * b + which] = jnp.concatenate([real, imag], axis=1).astype(BF16)

    sub = iota((8, 1), 0)
    for b in range(quads):
        sums = []
        for which in range(2):
            at = 2 * b + which
            _, _, points, first = plan.blocks[at]
            q, length = lengths[at]
            south = plan.lat - 1 - q
            lats = jnp.where(sub // 4 == 0, q, south)
            spin = 2.0 * cos_sin((2 * lats + 1).astype(F32), plan.lat * 1.0, plan.lat * 4.0)[0]
            angles = table[first : first + points, :]
            grid = lax.dot_general(coefs[at], angles, NT, preferred_element_type=F32)
            u, v, vort, temp = grid[0:8], grid[8:16], grid[16:24], grid[24:32]
            absolute = vort + spin
            inside = iota((1, points), 1).astype(F32) < length
            products = [absolute * u, absolute * v, 0.5 * (u * u + v * v), u * temp]
            products = jnp.concatenate([jnp.where(inside, p, 0.0) for p in products], axis=0).astype(BF16)
            back = jnp.dot(products, angles, preferred_element_type=F32)
            is_south = iota((32, 1), 0) // 4 % 2 == 1
            scale = jnp.where(is_south, quad[south], quad[q]) / length
            keep = open_[at]
            real = jnp.where(keep, back[:, 0:128] * scale, 0.0)
            imag = jnp.where(keep, -back[:, 128:256] * scale, 0.0)
            sums.append((real, imag))
        merged = jnp.concatenate([sums[0][0], sums[1][0], sums[0][1], sums[1][1]], axis=0).T
        for slot in range(2):
            stage[pl.ds(slot * quads + b, n, stride=ROWS), :] = merged[slot * n : (slot + 1) * n]
    ret_out[...] = stage[...].astype(BF16).reshape(n, ROWS, 128)

    def send_back(k, c):
        to = lax.rem(me + k, n)
        pltpu.make_async_remote_copy(
            ret_out.at[to], ret_in.at[me], ret_send, ret_recv, device_id={"wave": to}, device_id_type=MESH
        ).start()
        return c

    lax.fori_loop(1, n, send_back, 0)
    ret_in[me] = ret_out[me]

    def wait_level(k, acc):
        level_copy(k, lev).wait_recv()
        return acc + level_in[k]

    deeper = lax.fori_loop(lev + 1, depth, wait_level, jnp.zeros((4, span), F32))
    for slot in range(2):
        for part in range(2):
            at = slot * 2 + part
            below[slot, part] = below[slot, part] + deeper[at : at + 1]

    pltpu.make_async_copy(ret_in.at[others], ret_in.at[others], ret_recv).wait()
    stage[...] = ret_in[...].reshape(n * ROWS, 128).astype(F32)
    pick_row = iota((32, 128), 0)
    pick_col = iota((32, 128), 1)
    picked_of = (pick_row // 16) * 64 + (pick_row // 4 % 4) * 8 + pick_row % 4
    for slot in range(2):
        ahead = [stage[pl.ds(slot * quads + b, n, stride=ROWS), :].astype(BF16) for b in range(quads)]
        turned = [jnp.dot(flip, x, preferred_element_type=F32).astype(BF16) for x in ahead[::-1]]
        ahead = jnp.concatenate(ahead, axis=0)
        turned = jnp.concatenate(turned, axis=0)
        acc = jnp.zeros((32, span), F32)
        for k in range(4):
            which = 1 if k in (1, 2) else 0
            pick = (pick_col == picked_of + which * 32 + (k // 2) * 4).astype(BF16)
            left = lax.dot_general(pick, turned if k % 2 else ahead, NT, preferred_element_type=F32)
            acc = acc + jnp.dot(
                left.astype(BF16), leg[slot, k * quarter : (k + 1) * quarter, :], preferred_element_type=F32
            )
        zero = jnp.zeros((4, span), F32)
        geo = jnp.concatenate(
            [zero, zero, below[slot, 0], zero, zero, zero, below[slot, 1], zero], axis=0
        )
        live = column < span - waves[slot]
        out_ref[slot] = jnp.where(live, acc + geo, 0.0).astype(BF16)

    pltpu.make_async_copy(wave_rows.at[others], wave_rows.at[others], wave_send).wait()
    pltpu.make_async_copy(msg_out.at[others], msg_out.at[others], out_send).wait()
    pltpu.make_async_copy(ret_out.at[others], ret_out.at[others], ret_send).wait()

    def sent_level(k, c):
        level_copy(lev, k).wait_send()
        return c

    lax.fori_loop(0, lev, sent_level, 0)


def solution(mesh):
    plan = Plan(mesh)
    n, depth, span, lat = plan.groups, plan.depth, plan.span, plan.lat
    dma = pltpu.SemaphoreType.DMA

    def body(spec, legendre, layer_depth_share, quad_weight, wave_of_slot):
        any_spec = pl.BlockSpec(memory_space=pl.ANY)
        return pl.pallas_call(
            functools.partial(kernel, plan),
            out_shape=jax.ShapeDtypeStruct((2, 32, span), BF16),
            in_specs=[any_spec] * 5,
            out_specs=pl.BlockSpec(memory_space=pltpu.VMEM),
            scratch_shapes=[
                pltpu.VMEM((2, 32, span), BF16),
                pltpu.VMEM((2, lat, span), BF16),
                pltpu.SMEM((4,), F32),
                pltpu.SMEM((lat,), F32),
                pltpu.SMEM((2,), jnp.int32),
                pltpu.VMEM((1, 128), F32),
                pltpu.VMEM((n, 1, 128), F32),
                pltpu.VMEM((n * ROWS, 128), F32),
                pltpu.VMEM((n, ROWS, 128), BF16),
                pltpu.VMEM((n, ROWS, 128), BF16),
                pltpu.VMEM((n, ROWS, 128), BF16),
                pltpu.VMEM((n, ROWS, 128), BF16),
                pltpu.VMEM((2 * plan.quads, 32, 256), BF16),
                pltpu.VMEM((2 * plan.quads, 2, LOW + plan.coarse, 128), F32),
                pltpu.VMEM((plan.table_rows, 256), BF16),
                pltpu.VMEM((4, span), F32),
                pltpu.VMEM((depth, 4, span), F32),
                pltpu.VMEM((2, 2, 4, span), F32),
                dma((6,)), dma, dma, dma, dma, dma, dma, dma((depth,)), dma((depth,)),
            ],
            compiler_params=pltpu.CompilerParams(
                collective_id=0, has_side_effects=True, vmem_limit_bytes=60 * 1024 * 1024
            ),
        )(spec, legendre, layer_depth_share, quad_weight, wave_of_slot)

    in_specs = (P("wave", "lev", None), P("wave", None, None), P("lev"), P(), P("wave"))
    return jax.shard_map(body, mesh=mesh, in_specs=in_specs, out_specs=P("wave", "lev", None), check_vma=False)
```

```python
import functools
import math

import jax
import jax.numpy as jnp
from jax import lax
from jax.experimental import pallas as pl
from jax.experimental.pallas import tpu as pltpu
from jax.sharding import PartitionSpec as P

MESH = pl.DeviceIdType.MESH
F32 = jnp.float32
BF16 = jnp.bfloat16
ROWS = 16
LOW = 32
NT = (((1,), (1,)), ((), ()))


def round_up(x, step):
    return -(-x // step) * step


def iota(shape, dim):
    return lax.broadcasted_iota(jnp.int32, shape, dim)


def cos_sin(turns, quarter, length):
    count = jnp.floor(turns * (1.0 / quarter) + 0.5)
    x = (turns - count * quarter) * (2.0 * math.pi / length)
    y = x * x
    sine = x + x * y * (-1 / 6 + y * (1 / 120 + y * (-1 / 5040 + y * (1 / 362880))))
    cosine = 1.0 + y * (-0.5 + y * (1 / 24 + y * (-1 / 720 + y * (1 / 40320))))
    turn = count.astype(jnp.int32)
    swap = (turn & 1) == 1
    one = jnp.where(swap, sine, cosine)
    two = jnp.where(swap, cosine, sine)
    return jnp.where(((turn + 1) & 2) == 2, -one, one), jnp.where((turn & 2) == 2, -two, two)


class Plan:
    def __init__(self, mesh):
        self.groups = mesh.shape["wave"]
        self.depth = mesh.shape["lev"]
        self.lat = 1280
        self.span = 640
        self.quarter = self.lat // 4
        self.quads = self.quarter // self.groups
        self.blocks = []
        first = 0
        for quad in range(self.quads):
            low = quad * self.groups
            high = low + self.groups - 1
            for which in range(2):
                longest = 6 + (high if which == 0 else self.lat // 2 - 1 - low)
                points = round_up(longest, 128)
                self.blocks.append((quad, which, points, first))
                first += points
        self.table_rows = first
        self.coarse = round_up(max(b[2] for b in self.blocks) // LOW, 8)


def kernel(
    plan,
    spec_hbm, leg_hbm, share_hbm, quad_hbm, wave_hbm, out_ref,
    spec, leg, leg_turned, share, quad, waves,
    wave_row, wave_rows, stage, msg_out, msg_in, ret_out, ret_in,
    coefs, base, table, level_out, level_in, below,
    load_sem, wave_send, wave_recv, out_send, out_recv, ret_send, ret_recv, lev_send, lev_recv,
):
    n, depth, quads, span = plan.groups, plan.depth, plan.quads, plan.span
    me = lax.axis_index("wave")
    lev = lax.axis_index("lev")
    quarter = plan.quarter

    def partner(k):
        return lax.rem(me + n // 2 + (2 * (k % 2) - 1) * ((k + 1) // 2), n)

    barrier = pltpu.get_barrier_semaphore()

    def greet(k, c):
        pl.semaphore_signal(barrier, inc=1, device_id={"wave": partner(k)}, device_id_type=MESH)
        return c

    lax.fori_loop(0, n - 1, greet, 0)

    def greet_level(k, c):
        pl.semaphore_signal(barrier, inc=1, device_id={"lev": k}, device_id_type=MESH)
        return c

    lax.fori_loop(lev + 1, depth, greet_level, 0)

    loads = [
        pltpu.make_async_copy(wave_hbm, waves, load_sem.at[0]),
        pltpu.make_async_copy(spec_hbm, spec, load_sem.at[1]),
        pltpu.make_async_copy(share_hbm, share, load_sem.at[2]),
        pltpu.make_async_copy(quad_hbm, quad, load_sem.at[3]),
        pltpu.make_async_copy(leg_hbm.at[0], leg.at[0], load_sem.at[4]),
        pltpu.make_async_copy(leg_hbm.at[1], leg.at[1], load_sem.at[5]),
    ]
    for load in loads:
        load.start()
    loads[0].wait()
    lane = iota((1, 128), 1)
    row = jnp.where(lane == me, waves[0], 0) + jnp.where(lane == me + n, waves[1], 0)
    wave_row[...] = row.astype(F32)
    loads[1].wait()
    loads[2].wait()

    column = iota((1, span), 1)
    masked = []
    for slot in range(2):
        live = column < span - waves[slot]
        values = jnp.where(live, spec[slot].astype(F32), 0.0)
        masked.append(values.astype(BF16))
        for part in range(2):
            total = jnp.zeros((1, span), F32)
            for l in (3, 2, 1, 0):
                at = part * 16 + 12 + l
                total = total + values[at : at + 1] * share[l]
                below[slot, part, l : l + 1, :] = total
            level_out[slot * 2 + part : slot * 2 + part + 1, :] = total

    def which_of(k):
        return (k + 1) // 2 % 2

    where_row, where_col = iota((128, 32), 0), iota((128, 32), 1)
    column_of = (where_col // 16) * 64 + (where_col // 4 % 4) * 8 + where_col % 4
    place = [(where_row == column_of + which_of(k) * 32 + (k // 2) * 4).astype(BF16) for k in range(4)]
    flip = (iota((n, n), 0) + iota((n, n), 1) == n - 1).astype(BF16)

    def block(slot, k):
        if k % 2:
            return leg_turned[slot, k // 2]
        return leg[slot, k * quarter : (k + 1) * quarter, :]

    stage[...] = jnp.zeros_like(stage)
    for slot in range(2):
        loads[4 + slot].wait()
        for k in (1, 3):
            for b in range(quads):
                old = k * quarter + (quads - 1 - b) * n
                turned = jnp.dot(flip, leg[slot, old : old + n, :], preferred_element_type=F32)
                leg_turned[slot, k // 2, b * n : (b + 1) * n, :] = turned.astype(BF16)
        acc = None
        for k in range(4):
            weights = jnp.dot(place[k], masked[slot], preferred_element_type=F32).astype(BF16)
            term = lax.dot_general(block(slot, k), weights, NT, preferred_element_type=F32)
            acc = term if acc is None else acc + term
        for b in range(quads):
            stage[pl.ds(slot * quads + b, n, stride=ROWS), :] = acc[b * n : (b + 1) * n]
    msg_out[...] = stage[...].astype(BF16).reshape(n, ROWS, 128)

    pl.semaphore_wait(barrier, n - 1 + lev)

    def send_wave(k, c):
        pltpu.make_async_remote_copy(
            wave_row, wave_rows.at[me], wave_send, wave_recv,
            device_id={"wave": partner(k)}, device_id_type=MESH,
        ).start()
        return c

    lax.fori_loop(0, n - 1, send_wave, 0)

    def send_out(k, c):
        to = partner(k)
        pltpu.make_async_remote_copy(
            msg_out.at[to], msg_in.at[me], out_send, out_recv, device_id={"wave": to}, device_id_type=MESH
        ).start()
        return c

    lax.fori_loop(0, n - 1, send_out, 0)

    def level_copy(source, to):
        return pltpu.make_async_remote_copy(
            level_out, level_in.at[source], lev_send.at[to], lev_recv.at[source],
            device_id={"lev": to}, device_id_type=MESH,
        )

    def send_level(k, c):
        level_copy(lev, k).start()
        return c

    lax.fori_loop(0, lev, send_level, 0)
    wave_rows[me] = wave_row[...]
    msg_in[me] = msg_out[me]
    others = pl.ds(0, n - 1)
    loads[3].wait()
    pltpu.make_async_copy(wave_rows.at[others], wave_rows.at[others], wave_recv).wait()
    m = jnp.sum(wave_rows[...], axis=0)

    index = iota((LOW + plan.coarse, 1), 0)
    step = jnp.where(index < LOW, index, (index - LOW) * LOW).astype(F32)
    turns = step * m
    lengths = []
    for at, (b, which, points, first) in enumerate(plan.blocks):
        q = me + b * n
        if which == 1:
            q = plan.lat // 2 - 1 - q
        quart = (5 + q).astype(F32)
        lengths.append((q, quart, quart * 4.0))
        c, s = cos_sin(turns, quart, quart * 4.0)
        base[at, 0] = c
        base[at, 1] = s
    for at, (b, which, points, first) in enumerate(plan.blocks):
        cl, sl = base[at, 0, 0:LOW, :], base[at, 1, 0:LOW, :]
        for a in range(points // LOW):
            ch, sh = base[at, 0, LOW + a : LOW + a + 1, :], base[at, 1, LOW + a : LOW + a + 1, :]
            to = first + a * LOW
            table[to : to + LOW, 0:128] = (ch * cl - sh * sl).astype(BF16)
            table[to : to + LOW, 128:256] = (sh * cl + ch * sl).astype(BF16)

    pltpu.make_async_copy(msg_in.at[others], msg_in.at[others], out_recv).wait()
    stage[...] = msg_in[...].reshape(n * ROWS, 128).astype(F32)
    double = jnp.where(m == 0.0, 1.0, 2.0)
    parity = 1.0 - 2.0 * (m - 2.0 * jnp.floor(m * 0.5))
    keep = [2.0 * m < length for _, _, length in lengths]
    none = jnp.zeros((32, 128), F32)
    for b in range(quads):
        rows_in = [stage[pl.ds(slot * quads + b, n, stride=ROWS), :] for slot in range(2)]
        turned = jnp.concatenate(rows_in, axis=0).T
        for which in range(2):
            amplitude = jnp.where(keep[2 * b + which], double, 0.0)
            real = turned[which * 32 : which * 32 + 32] * amplitude
            imag = turned[64 + which * 32 : 96 + which * 32] * amplitude
            left = jnp.concatenate([real, none, real * parity, none], axis=0)
            right = jnp.concatenate([none, imag, none, imag * -parity], axis=0)
            coefs[2 * b + which] = jnp.concatenate([left, right], axis=1).astype(BF16)

    sub = iota((8, 1), 0)
    for b in range(quads):
        sums = []
        for which in range(2):
            at = 2 * b + which
            _, _, points, first = plan.blocks[at]
            q, quart, length = lengths[at]
            south = plan.lat - 1 - q
            lats = jnp.where(sub // 4 == 0, q, south)
            spin = 2.0 * cos_sin((2 * lats + 1).astype(F32), plan.lat * 1.0, plan.lat * 4.0)[0]
            angles = table[first : first + points, :]
            sides = lax.dot_general(coefs[at], angles, NT, preferred_element_type=F32)
            even, odd, even2, odd2 = (sides[32 * i : 32 * i + 32] for i in range(4))
            point = iota((1, points), 1).astype(F32)
            below_end = point < quart
            up_to_end = point <= quart
            later = point > 0.0
            products = []
            for grid, inside in (
                (even - odd, up_to_end),
                (even + odd, up_to_end & later),
                (even2 - odd2, below_end),
                (even2 + odd2, below_end & later),
            ):
                u, v, vort, temp = grid[0:8], grid[8:16], grid[16:24], grid[24:32]
                absolute = vort + spin
                for p in (absolute * u, absolute * v, 0.5 * (u * u + v * v), u * temp):
                    products.append(jnp.where(inside, p, 0.0))
            products = jnp.concatenate(products, axis=0).astype(BF16)
            back = jnp.dot(products, angles, preferred_element_type=F32)
            b1, b2, b3, b4 = (back[32 * i : 32 * i + 32] for i in range(4))
            real = (b1 + b2)[:, 0:128] + parity * (b3 + b4)[:, 0:128]
            imag = (b2 - b1)[:, 128:256] + parity * (b3 - b4)[:, 128:256]
            is_south = iota((32, 1), 0) // 4 % 2 == 1
            scale = jnp.where(is_south, quad[south], quad[q]) / length
            sums.append((jnp.where(keep[at], real * scale, 0.0), jnp.where(keep[at], imag * scale, 0.0)))
        merged = jnp.concatenate([sums[0][0], sums[1][0], sums[0][1], sums[1][1]], axis=0).T
        for slot in range(2):
            stage[pl.ds(slot * quads + b, n, stride=ROWS), :] = merged[slot * n : (slot + 1) * n]
    ret_out[...] = stage[...].astype(BF16).reshape(n, ROWS, 128)

    def send_back(k, c):
        to = partner(k)
        pltpu.make_async_remote_copy(
            ret_out.at[to], ret_in.at[me], ret_send, ret_recv, device_id={"wave": to}, device_id_type=MESH
        ).start()
        return c

    lax.fori_loop(0, n - 1, send_back, 0)
    ret_in[me] = ret_out[me]

    def wait_level(k, acc):
        level_copy(k, lev).wait_recv()
        return acc + level_in[k]

    deeper = lax.fori_loop(lev + 1, depth, wait_level, jnp.zeros((4, span), F32))
    for slot in range(2):
        for part in range(2):
            at = slot * 2 + part
            below[slot, part] = below[slot, part] + deeper[at : at + 1]
    row_of = iota((128, 128), 0)
    picked_of = (row_of // 16 % 2) * 64 + (row_of // 4 % 4) * 8 + row_of % 4
    picked_of = picked_of + which_of(row_of // 32) * 32 + (row_of // 64) * 4
    pick = (iota((128, 128), 1) == picked_of).astype(BF16)

    pltpu.make_async_copy(ret_in.at[others], ret_in.at[others], ret_recv).wait()
    stage[...] = ret_in[...].reshape(n * ROWS, 128).astype(F32)
    for slot in range(2):
        rows_in = [stage[pl.ds(slot * quads + b, n, stride=ROWS), :] for b in range(quads)]
        rows_in = jnp.concatenate(rows_in, axis=0).astype(BF16)
        left = lax.dot_general(pick, rows_in, NT, preferred_element_type=F32).astype(BF16)
        zero = jnp.zeros((4, span), F32)
        acc = jnp.concatenate([zero, zero, below[slot, 0], zero, zero, zero, below[slot, 1], zero], axis=0)
        for k in range(4):
            acc = acc + jnp.dot(left[k * 32 : k * 32 + 32], block(slot, k), preferred_element_type=F32)
        live = column < span - waves[slot]
        out_ref[slot] = jnp.where(live, acc, 0.0).astype(BF16)

    pltpu.make_async_copy(wave_rows.at[others], wave_rows.at[others], wave_send).wait()
    pltpu.make_async_copy(msg_out.at[others], msg_out.at[others], out_send).wait()
    pltpu.make_async_copy(ret_out.at[others], ret_out.at[others], ret_send).wait()

    def sent_level(k, c):
        level_copy(lev, k).wait_send()
        return c

    lax.fori_loop(0, lev, sent_level, 0)


def solution(mesh):
    plan = Plan(mesh)
    n, depth, span, lat = plan.groups, plan.depth, plan.span, plan.lat
    dma = pltpu.SemaphoreType.DMA

    def body(spec, legendre, layer_depth_share, quad_weight, wave_of_slot):
        any_spec = pl.BlockSpec(memory_space=pltpu.HBM)
        return pl.pallas_call(
            functools.partial(kernel, plan),
            out_shape=jax.ShapeDtypeStruct((2, 32, span), BF16),
            in_specs=[any_spec] * 5,
            out_specs=pl.BlockSpec(memory_space=pltpu.VMEM),
            scratch_shapes=[
                pltpu.VMEM((2, 32, span), BF16),
                pltpu.VMEM((2, lat, span), BF16),
                pltpu.VMEM((2, 2, lat // 4, span), BF16),
                pltpu.SMEM((4,), F32),
                pltpu.SMEM((lat,), F32),
                pltpu.SMEM((2,), jnp.int32),
                pltpu.VMEM((1, 128), F32),
                pltpu.VMEM((n, 1, 128), F32),
                pltpu.VMEM((n * ROWS, 128), F32),
                pltpu.VMEM((n, ROWS, 128), BF16),
                pltpu.VMEM((n, ROWS, 128), BF16),
                pltpu.VMEM((n, ROWS, 128), BF16),
                pltpu.VMEM((n, ROWS, 128), BF16),
                pltpu.VMEM((2 * plan.quads, 128, 256), BF16),
                pltpu.VMEM((2 * plan.quads, 2, LOW + plan.coarse, 128), F32),
                pltpu.VMEM((plan.table_rows, 256), BF16),
                pltpu.VMEM((4, span), F32),
                pltpu.VMEM((depth, 4, span), F32),
                pltpu.VMEM((2, 2, 4, span), F32),
                dma((6,)), dma, dma, dma, dma, dma, dma, dma((depth,)), dma((depth,)),
            ],
            compiler_params=pltpu.CompilerParams(
                collective_id=0, has_side_effects=True, vmem_limit_bytes=63 * 1024 * 1024
            ),
        )(spec, legendre, layer_depth_share, quad_weight, wave_of_slot)

    in_specs = (P("wave", "lev", None), P("wave", None, None), P("lev"), P(), P("wave"))
    return jax.shard_map(body, mesh=mesh, in_specs=in_specs, out_specs=P("wave", "lev", None), check_vma=False)
```

```python
import functools
import math

import jax
import jax.numpy as jnp
from jax import lax
from jax.experimental import pallas as pl
from jax.experimental.pallas import tpu as pltpu
from jax.sharding import PartitionSpec as P

MESH = pl.DeviceIdType.MESH
F32 = jnp.float32
BF16 = jnp.bfloat16
LOW = 32
NT = (((1,), (1,)), ((), ()))


def round_up(x, step):
    return -(-x // step) * step


def iota(shape, dim):
    return lax.broadcasted_iota(jnp.int32, shape, dim)


def cos_sin(turns, quarter, length):
    count = jnp.floor(turns * (1.0 / quarter) + 0.5)
    x = (turns - count * quarter) * (2.0 * math.pi / length)
    y = x * x
    sine = x + x * y * (-1 / 6 + y * (1 / 120 + y * (-1 / 5040 + y * (1 / 362880))))
    cosine = 1.0 + y * (-0.5 + y * (1 / 24 + y * (-1 / 720 + y * (1 / 40320))))
    turn = count.astype(jnp.int32)
    swap = (turn & 1) == 1
    one = jnp.where(swap, sine, cosine)
    two = jnp.where(swap, cosine, sine)
    return jnp.where(((turn + 1) & 2) == 2, -one, one), jnp.where((turn & 2) == 2, -two, two)


class Plan:
    def __init__(self, mesh):
        self.groups = mesh.shape["wave"]
        self.depth = mesh.shape["lev"]
        self.lat = 1280
        self.span = 640
        self.quarter = self.lat // 4
        self.quads = self.quarter // self.groups
        self.rows = 2 * self.quads
        self.blocks = []
        first = 0
        for quad in range(self.quads):
            low = quad * self.groups
            high = low + self.groups - 1
            for which in range(2):
                longest = 6 + (high if which == 0 else self.lat // 2 - 1 - low)
                points = round_up(longest, 128)
                self.blocks.append((quad, which, points, first))
                first += points
        self.table_rows = first
        self.coarse = round_up(max(b[2] for b in self.blocks) // LOW, 8)


def kernel(
    plan,
    spec_hbm, leg_hbm, share_hbm, quad_hbm, wave_hbm, out_ref,
    spec, leg, leg_turned, share, quad, waves,
    wave_row, wave_rows, stage, msg_out, msg_in, ret_out, ret_in,
    coefs, base, table, level_out, level_in, below,
    load_sem, wave_send, wave_recv, out_send, out_recv, ret_send, ret_recv, lev_send, lev_recv,
):
    n, depth, quads, span = plan.groups, plan.depth, plan.quads, plan.span
    me = lax.axis_index("wave")
    lev = lax.axis_index("lev")
    quarter, rows = plan.quarter, plan.rows

    def partner(k):
        return lax.rem(me + n // 2 + (2 * (k % 2) - 1) * ((k + 1) // 2), n)

    def message(ref, k):
        return ref.at[pl.ds(pl.multiple_of(k * rows, 2), rows)]

    barrier = pltpu.get_barrier_semaphore()

    def greet(k, c):
        pl.semaphore_signal(barrier, inc=1, device_id={"wave": partner(k)}, device_id_type=MESH)
        return c

    lax.fori_loop(0, n - 1, greet, 0)

    def greet_level(k, c):
        pl.semaphore_signal(barrier, inc=1, device_id={"lev": k}, device_id_type=MESH)
        return c

    lax.fori_loop(lev + 1, depth, greet_level, 0)

    loads = [
        pltpu.make_async_copy(wave_hbm, waves, load_sem.at[0]),
        pltpu.make_async_copy(spec_hbm, spec, load_sem.at[1]),
        pltpu.make_async_copy(share_hbm, share, load_sem.at[2]),
        pltpu.make_async_copy(quad_hbm, quad, load_sem.at[3]),
        pltpu.make_async_copy(leg_hbm.at[0], leg.at[0], load_sem.at[4]),
        pltpu.make_async_copy(leg_hbm.at[1], leg.at[1], load_sem.at[5]),
    ]
    for load in loads:
        load.start()
    loads[0].wait()
    lane = iota((1, 128), 1)
    row = jnp.where(lane == me, waves[0], 0) + jnp.where(lane == me + n, waves[1], 0)
    wave_row[...] = row.astype(F32)
    loads[1].wait()
    loads[2].wait()

    column = iota((1, span), 1)
    masked = []
    for slot in range(2):
        live = column < span - waves[slot]
        values = jnp.where(live, spec[slot].astype(F32), 0.0)
        masked.append(values.astype(BF16))
        for part in range(2):
            total = jnp.zeros((1, span), F32)
            for l in (3, 2, 1, 0):
                at = part * 16 + 12 + l
                total = total + values[at : at + 1] * share[l]
                below[slot, part, l : l + 1, :] = total
            level_out[slot * 2 + part : slot * 2 + part + 1, :] = total

    def which_of(k):
        return (k + 1) // 2 % 2

    where_row, where_col = iota((128, 32), 0), iota((128, 32), 1)
    column_of = (where_col // 16) * 64 + (where_col // 4 % 4) * 8 + where_col % 4
    place = [(where_row == column_of + which_of(k) * 32 + (k // 2) * 4).astype(BF16) for k in range(4)]
    flip = (iota((n, n), 0) + iota((n, n), 1) == n - 1).astype(BF16)

    def block(slot, k):
        if k % 2:
            return leg_turned[slot, k // 2]
        return leg[slot, k * quarter : (k + 1) * quarter, :]

    for slot in range(2):
        loads[4 + slot].wait()
        for k in (1, 3):
            for b in range(quads):
                old = k * quarter + (quads - 1 - b) * n
                turned = jnp.dot(flip, leg[slot, old : old + n, :], preferred_element_type=F32)
                leg_turned[slot, k // 2, b * n : (b + 1) * n, :] = turned.astype(BF16)
        acc = None
        for k in range(4):
            weights = jnp.dot(place[k], masked[slot], preferred_element_type=F32).astype(BF16)
            term = lax.dot_general(block(slot, k), weights, NT, preferred_element_type=F32)
            acc = term if acc is None else acc + term
        for b in range(quads):
            stage[pl.ds(slot * quads + b, n, stride=rows), :] = acc[b * n : (b + 1) * n]
    msg_out[...] = stage[...].astype(BF16)

    pl.semaphore_wait(barrier, n - 1 + lev)

    def send_wave(k, c):
        pltpu.make_async_remote_copy(
            wave_row, wave_rows.at[me], wave_send, wave_recv,
            device_id={"wave": partner(k)}, device_id_type=MESH,
        ).start()
        return c

    lax.fori_loop(0, n - 1, send_wave, 0)

    def send_out(k, c):
        to = partner(k)
        pltpu.make_async_remote_copy(
            message(msg_out, to), message(msg_in, me), out_send, out_recv, device_id={"wave": to}, device_id_type=MESH
        ).start()
        return c

    lax.fori_loop(0, n - 1, send_out, 0)

    def level_copy(source, to):
        return pltpu.make_async_remote_copy(
            level_out, level_in.at[source], lev_send.at[to], lev_recv.at[source],
            device_id={"lev": to}, device_id_type=MESH,
        )

    def send_level(k, c):
        level_copy(lev, k).start()
        return c

    lax.fori_loop(0, lev, send_level, 0)
    wave_rows[me] = wave_row[...]
    pltpu.make_async_copy(message(msg_out, me), message(msg_in, me), out_recv).start()
    others, most = pl.ds(0, n - 1), pl.ds(0, (n - 1) * rows)
    loads[3].wait()
    pltpu.make_async_copy(wave_rows.at[others], wave_rows.at[others], wave_recv).wait()
    m = jnp.sum(wave_rows[...], axis=0)

    index = iota((LOW + plan.coarse, 1), 0)
    step = jnp.where(index < LOW, index, (index - LOW) * LOW).astype(F32)
    turns = step * m
    lengths = []
    for at, (b, which, points, first) in enumerate(plan.blocks):
        q = me + b * n
        if which == 1:
            q = plan.lat // 2 - 1 - q
        quart = (5 + q).astype(F32)
        lengths.append((q, quart, quart * 4.0))
        c, s = cos_sin(turns, quart, quart * 4.0)
        base[at, 0] = c
        base[at, 1] = s
    for at, (b, which, points, first) in enumerate(plan.blocks):
        cl, sl = base[at, 0, 0:LOW, :], base[at, 1, 0:LOW, :]
        for a in range(points // LOW):
            ch, sh = base[at, 0, LOW + a : LOW + a + 1, :], base[at, 1, LOW + a : LOW + a + 1, :]
            to = first + a * LOW
            table[to : to + LOW, 0:128] = (ch * cl - sh * sl).astype(BF16)
            table[to : to + LOW, 128:256] = (sh * cl + ch * sl).astype(BF16)

    pltpu.make_async_copy(msg_in, msg_in, out_recv).wait()
    stage[...] = msg_in[...].astype(F32)
    double = jnp.where(m == 0.0, 1.0, 2.0)
    parity = 1.0 - 2.0 * (m - 2.0 * jnp.floor(m * 0.5))
    keep = [2.0 * m < length for _, _, length in lengths]
    none = jnp.zeros((32, 128), F32)
    for b in range(quads):
        rows_in = [stage[pl.ds(slot * quads + b, n, stride=rows), :] for slot in range(2)]
        turned = jnp.concatenate(rows_in, axis=0).T
        for which in range(2):
            amplitude = jnp.where(keep[2 * b + which], double, 0.0)
            real = turned[which * 32 : which * 32 + 32] * amplitude
            imag = turned[64 + which * 32 : 96 + which * 32] * amplitude
            left = jnp.concatenate([real, none, real * parity, none], axis=0)
            right = jnp.concatenate([none, imag, none, imag * -parity], axis=0)
            coefs[2 * b + which] = jnp.concatenate([left, right], axis=1).astype(BF16)

    sub = iota((8, 1), 0)
    for b in range(quads):
        sums = []
        for which in range(2):
            at = 2 * b + which
            _, _, points, first = plan.blocks[at]
            q, quart, length = lengths[at]
            south = plan.lat - 1 - q
            lats = jnp.where(sub // 4 == 0, q, south)
            spin = 2.0 * cos_sin((2 * lats + 1).astype(F32), plan.lat * 1.0, plan.lat * 4.0)[0]
            angles = table[first : first + points, :]
            sides = lax.dot_general(coefs[at], angles, NT, preferred_element_type=F32)
            even, odd, even2, odd2 = (sides[32 * i : 32 * i + 32] for i in range(4))
            point = iota((1, points), 1).astype(F32)
            below_end = point < quart
            up_to_end = point <= quart
            later = point > 0.0
            products = []
            for grid, inside in (
                (even - odd, up_to_end),
                (even + odd, up_to_end & later),
                (even2 - odd2, below_end),
                (even2 + odd2, below_end & later),
            ):
                u, v, vort, temp = grid[0:8], grid[8:16], grid[16:24], grid[24:32]
                absolute = vort + spin
                for p in (absolute * u, absolute * v, 0.5 * (u * u + v * v), u * temp):
                    products.append(jnp.where(inside, p, 0.0))
            products = jnp.concatenate(products, axis=0).astype(BF16)
            back = jnp.dot(products, angles, preferred_element_type=F32)
            b1, b2, b3, b4 = (back[32 * i : 32 * i + 32] for i in range(4))
            real = (b1 + b2)[:, 0:128] + parity * (b3 + b4)[:, 0:128]
            imag = (b2 - b1)[:, 128:256] + parity * (b3 - b4)[:, 128:256]
            is_south = iota((32, 1), 0) // 4 % 2 == 1
            scale = jnp.where(is_south, quad[south], quad[q]) / length
            sums.append((jnp.where(keep[at], real * scale, 0.0), jnp.where(keep[at], imag * scale, 0.0)))
        merged = jnp.concatenate([sums[0][0], sums[1][0], sums[0][1], sums[1][1]], axis=0).T
        for slot in range(2):
            stage[pl.ds(slot * quads + b, n, stride=rows), :] = merged[slot * n : (slot + 1) * n]
    ret_out[...] = stage[...].astype(BF16)

    def send_back(k, c):
        to = partner(k)
        pltpu.make_async_remote_copy(
            message(ret_out, to), message(ret_in, me), ret_send, ret_recv, device_id={"wave": to}, device_id_type=MESH
        ).start()
        return c

    lax.fori_loop(0, n - 1, send_back, 0)
    pltpu.make_async_copy(message(ret_out, me), message(ret_in, me), ret_recv).start()

    def wait_level(k, acc):
        level_copy(k, lev).wait_recv()
        return acc + level_in[k]

    deeper = lax.fori_loop(lev + 1, depth, wait_level, jnp.zeros((4, span), F32))
    for slot in range(2):
        for part in range(2):
            at = slot * 2 + part
            below[slot, part] = below[slot, part] + deeper[at : at + 1]
    row_of = iota((128, 128), 0)
    picked_of = (row_of // 16 % 2) * 64 + (row_of // 4 % 4) * 8 + row_of % 4
    picked_of = picked_of + which_of(row_of // 32) * 32 + (row_of // 64) * 4
    pick = (iota((128, 128), 1) == picked_of).astype(BF16)

    pltpu.make_async_copy(ret_in, ret_in, ret_recv).wait()
    stage[...] = ret_in[...].astype(F32)
    for slot in range(2):
        rows_in = [stage[pl.ds(slot * quads + b, n, stride=rows), :] for b in range(quads)]
        rows_in = jnp.concatenate(rows_in, axis=0).astype(BF16)
        left = lax.dot_general(pick, rows_in, NT, preferred_element_type=F32).astype(BF16)
        zero = jnp.zeros((4, span), F32)
        acc = jnp.concatenate([zero, zero, below[slot, 0], zero, zero, zero, below[slot, 1], zero], axis=0)
        for k in range(4):
            acc = acc + jnp.dot(left[k * 32 : k * 32 + 32], block(slot, k), preferred_element_type=F32)
        live = column < span - waves[slot]
        out_ref[slot] = jnp.where(live, acc, 0.0).astype(BF16)

    pltpu.make_async_copy(wave_rows.at[others], wave_rows.at[others], wave_send).wait()
    pltpu.make_async_copy(msg_out.at[most], msg_out.at[most], out_send).wait()
    pltpu.make_async_copy(ret_out.at[most], ret_out.at[most], ret_send).wait()

    def sent_level(k, c):
        level_copy(lev, k).wait_send()
        return c

    lax.fori_loop(0, lev, sent_level, 0)


def solution(mesh):
    plan = Plan(mesh)
    n, depth, span, lat = plan.groups, plan.depth, plan.span, plan.lat
    dma = pltpu.SemaphoreType.DMA

    def body(*args):
        any_spec = pl.BlockSpec(memory_space=pltpu.HBM)
        return pl.pallas_call(
            functools.partial(kernel, plan),
            out_shape=jax.ShapeDtypeStruct((2, 32, span), BF16),
            in_specs=[any_spec] * 5,
            out_specs=pl.BlockSpec(memory_space=pltpu.VMEM),
            scratch_shapes=[
                pltpu.VMEM((2, 32, span), BF16),
                pltpu.VMEM((2, lat, span), BF16),
                pltpu.VMEM((2, 2, lat // 4, span), BF16),
                pltpu.SMEM((4,), F32),
                pltpu.SMEM((lat,), F32),
                pltpu.SMEM((2,), jnp.int32),
                pltpu.VMEM((1, 128), F32),
                pltpu.VMEM((n, 1, 128), F32),
                pltpu.VMEM((n * plan.rows, 128), F32),
                pltpu.VMEM((n * plan.rows, 128), BF16),
                pltpu.VMEM((n * plan.rows, 128), BF16),
                pltpu.VMEM((n * plan.rows, 128), BF16),
                pltpu.VMEM((n * plan.rows, 128), BF16),
                pltpu.VMEM((2 * plan.quads, 128, 256), BF16),
                pltpu.VMEM((2 * plan.quads, 2, LOW + plan.coarse, 128), F32),
                pltpu.VMEM((plan.table_rows, 256), BF16),
                pltpu.VMEM((4, span), F32),
                pltpu.VMEM((depth, 4, span), F32),
                pltpu.VMEM((2, 2, 4, span), F32),
                dma((6,)), dma, dma, dma, dma, dma, dma, dma((depth,)), dma((depth,)),
            ],
            compiler_params=pltpu.CompilerParams(
                collective_id=0, has_side_effects=True, vmem_limit_bytes=24 * 1024 * 1024
            ),
        )(*[pltpu.with_memory_space_constraint(x, pltpu.HBM) for x in args])

    in_specs = (P("wave", "lev", None), P("wave", None, None), P("lev"), P(), P("wave"))
    return jax.shard_map(body, mesh=mesh, in_specs=in_specs, out_specs=P("wave", "lev", None), check_vma=False)
```

```python
import functools
import math

import jax
import jax.numpy as jnp
from jax import lax
from jax.experimental import pallas as pl
from jax.experimental.pallas import tpu as pltpu
from jax.sharding import PartitionSpec as P

MESH = pl.DeviceIdType.MESH
F32 = jnp.float32
BF16 = jnp.bfloat16
LOW = 32
NT = (((1,), (1,)), ((), ()))


def round_up(x, step):
    return -(-x // step) * step


def iota(shape, dim):
    return lax.broadcasted_iota(jnp.int32, shape, dim)


def cos_sin(turns, quarter, length):
    count = jnp.floor(turns * (1.0 / quarter) + 0.5)
    x = (turns - count * quarter) * (2.0 * math.pi / length)
    y = x * x
    sine = x + x * y * (-1 / 6 + y * (1 / 120 + y * (-1 / 5040 + y * (1 / 362880))))
    cosine = 1.0 + y * (-0.5 + y * (1 / 24 + y * (-1 / 720 + y * (1 / 40320))))
    turn = count.astype(jnp.int32)
    swap = (turn & 1) == 1
    one = jnp.where(swap, sine, cosine)
    two = jnp.where(swap, cosine, sine)
    return jnp.where(((turn + 1) & 2) == 2, -one, one), jnp.where((turn & 2) == 2, -two, two)


class Plan:
    def __init__(self, mesh):
        self.groups = mesh.shape["wave"]
        self.depth = mesh.shape["lev"]
        self.lat = 1280
        self.span = 640
        self.quarter = self.lat // 4
        self.quads = self.quarter // self.groups
        self.rows = 2 * self.quads
        self.blocks = []
        first = 0
        for quad in range(self.quads):
            low = quad * self.groups
            high = low + self.groups - 1
            for which in range(2):
                longest = 6 + (high if which == 0 else self.lat // 2 - 1 - low)
                points = round_up(longest, 128)
                self.blocks.append((quad, which, points, first))
                first += points
        self.table_rows = first
        self.coarse = round_up(max(b[2] for b in self.blocks) // LOW, 8)


def kernel(
    plan,
    spec_hbm, leg_hbm, share_hbm, quad_hbm, wave_hbm, out_ref,
    spec, leg, leg_turned, share, quad, waves,
    wave_row, wave_rows, stage, msg_out, msg_in, ret_out, ret_in,
    coefs, base, table, level_out, level_in, below,
    load_sem, wave_send, wave_recv, out_send, out_recv, ret_send, ret_recv, lev_send, lev_recv,
):
    n, depth, quads, span = plan.groups, plan.depth, plan.quads, plan.span
    me = lax.axis_index("wave")
    lev = lax.axis_index("lev")
    quarter, rows = plan.quarter, plan.rows

    def partners(visit):
        def at(offset):
            to = me + offset
            visit(jnp.where(to >= n, to - n, to))

        def both(p):
            at(n // 2 - p)
            at(n // 2 + p)

        def several(i, c):
            for u in range(3):
                both(3 * i + u + 1)
            return c

        at(n // 2)
        lax.fori_loop(0, (n // 2 - 1) // 3, several, 0)
        for p in range((n // 2 - 1) // 3 * 3 + 1, n // 2):
            both(p)

    def message(ref, k):
        return ref.at[pl.ds(pl.multiple_of(k * rows, 2), rows)]

    loads = [
        pltpu.make_async_copy(wave_hbm, waves, load_sem.at[0]),
        pltpu.make_async_copy(spec_hbm, spec, load_sem.at[1]),
        pltpu.make_async_copy(share_hbm, share, load_sem.at[2]),
        pltpu.make_async_copy(quad_hbm, quad, load_sem.at[3]),
        pltpu.make_async_copy(leg_hbm.at[0], leg.at[0], load_sem.at[4]),
        pltpu.make_async_copy(leg_hbm.at[1], leg.at[1], load_sem.at[5]),
    ]
    for load in loads:
        load.start()

    barrier = pltpu.get_barrier_semaphore()

    def greet(to):
        pl.semaphore_signal(barrier, inc=1, device_id={"wave": to}, device_id_type=MESH)

    partners(greet)

    def greet_level(k, c):
        pl.semaphore_signal(barrier, inc=1, device_id={"lev": k}, device_id_type=MESH)
        return c

    lax.fori_loop(lev + 1, depth, greet_level, 0)

    loads[0].wait()
    lane = iota((1, 128), 1)
    row = jnp.where(lane == me, waves[0], 0) + jnp.where(lane == me + n, waves[1], 0)
    wave_row[...] = row.astype(F32)
    loads[1].wait()
    loads[2].wait()

    column = iota((1, span), 1)
    masked = []
    for slot in range(2):
        live = column < span - waves[slot]
        values = jnp.where(live, spec[slot].astype(F32), 0.0)
        masked.append(values.astype(BF16))
        for part in range(2):
            total = jnp.zeros((1, span), F32)
            for l in (3, 2, 1, 0):
                at = part * 16 + 12 + l
                total = total + values[at : at + 1] * share[l]
                below[slot, part, l : l + 1, :] = total
            level_out[slot * 2 + part : slot * 2 + part + 1, :] = total

    def which_of(k):
        return (k + 1) // 2 % 2

    where_row, where_col = iota((128, 32), 0), iota((128, 32), 1)
    column_of = (where_col // 16) * 64 + (where_col // 4 % 4) * 8 + where_col % 4
    place = [(where_row == column_of + which_of(k) * 32 + (k // 2) * 4).astype(BF16) for k in range(4)]
    flip = (iota((n, n), 0) + iota((n, n), 1) == n - 1).astype(BF16)

    def block(slot, k):
        if k % 2:
            return leg_turned[slot, k // 2]
        return leg[slot, k * quarter : (k + 1) * quarter, :]

    for slot in range(2):
        loads[4 + slot].wait()
        for k in (1, 3):
            for b in range(quads):
                old = k * quarter + (quads - 1 - b) * n
                turned = jnp.dot(flip, leg[slot, old : old + n, :], preferred_element_type=F32)
                leg_turned[slot, k // 2, b * n : (b + 1) * n, :] = turned.astype(BF16)
        acc = None
        for k in range(4):
            weights = jnp.dot(place[k], masked[slot], preferred_element_type=F32).astype(BF16)
            term = lax.dot_general(block(slot, k), weights, NT, preferred_element_type=F32)
            acc = term if acc is None else acc + term
        for b in range(quads):
            stage[pl.ds(slot * quads + b, n, stride=rows), :] = acc[b * n : (b + 1) * n]
    msg_out[...] = stage[...].astype(BF16)

    pl.semaphore_wait(barrier, n - 1 + lev)

    def send_wave(to):
        pltpu.make_async_remote_copy(
            wave_row, wave_rows.at[pl.ds(me, 1)], wave_send, wave_recv, device_id={"wave": to}, device_id_type=MESH
        ).start()

    partners(send_wave)

    def send_out(to):
        pltpu.make_async_remote_copy(
            message(msg_out, to), message(msg_in, me), out_send, out_recv, device_id={"wave": to}, device_id_type=MESH
        ).start()

    partners(send_out)

    def level_copy(source, to):
        return pltpu.make_async_remote_copy(
            level_out, level_in.at[source], lev_send.at[to], lev_recv.at[source],
            device_id={"lev": to}, device_id_type=MESH,
        )

    def send_level(k, c):
        level_copy(lev, k).start()
        return c

    lax.fori_loop(0, lev, send_level, 0)
    pltpu.make_async_copy(wave_row, wave_rows.at[pl.ds(me, 1)], wave_recv).start()
    pltpu.make_async_copy(message(msg_out, me), message(msg_in, me), out_recv).start()
    others, most = pl.ds(0, n - 1), pl.ds(0, (n - 1) * rows)
    loads[3].wait()
    pltpu.make_async_copy(wave_rows, wave_rows, wave_recv).wait()
    m = jnp.sum(wave_rows[...], axis=0, keepdims=True)

    index = iota((LOW + plan.coarse, 1), 0)
    step = jnp.where(index < LOW, index, (index - LOW) * LOW).astype(F32)
    turns = step * m
    lengths = []
    for at, (b, which, points, first) in enumerate(plan.blocks):
        q = me + b * n
        if which == 1:
            q = plan.lat // 2 - 1 - q
        quart = (5 + q).astype(F32)
        lengths.append((q, quart, quart * 4.0))
        c, s = cos_sin(turns, quart, quart * 4.0)
        base[at, 0] = c
        base[at, 1] = s
    for at, (b, which, points, first) in enumerate(plan.blocks):
        cl, sl = base[at, 0, 0:LOW, :], base[at, 1, 0:LOW, :]
        for a in range(points // LOW):
            ch, sh = base[at, 0, LOW + a : LOW + a + 1, :], base[at, 1, LOW + a : LOW + a + 1, :]
            to = first + a * LOW
            table[to : to + LOW, 0:128] = (ch * cl - sh * sl).astype(BF16)
            table[to : to + LOW, 128:256] = (sh * cl + ch * sl).astype(BF16)

    pltpu.make_async_copy(msg_in, msg_in, out_recv).wait()
    stage[...] = msg_in[...].astype(F32)
    double = jnp.where(m == 0.0, 1.0, 2.0)
    parity = 1.0 - 2.0 * (m - 2.0 * jnp.floor(m * 0.5))
    keep = [2.0 * m < length for _, _, length in lengths]
    none = jnp.zeros((32, 128), F32)
    for b in range(quads):
        rows_in = [stage[pl.ds(slot * quads + b, n, stride=rows), :] for slot in range(2)]
        turned = jnp.concatenate(rows_in, axis=0).T
        for which in range(2):
            amplitude = jnp.where(keep[2 * b + which], double, 0.0)
            real = turned[which * 32 : which * 32 + 32] * amplitude
            imag = turned[64 + which * 32 : 96 + which * 32] * amplitude
            left = jnp.concatenate([real, none, real * parity, none], axis=0)
            right = jnp.concatenate([none, imag, none, imag * -parity], axis=0)
            coefs[2 * b + which] = jnp.concatenate([left, right], axis=1).astype(BF16)

    sub = iota((8, 1), 0)
    for b in range(quads):
        sums = []
        for which in range(2):
            at = 2 * b + which
            _, _, points, first = plan.blocks[at]
            q, quart, length = lengths[at]
            south = plan.lat - 1 - q
            lats = jnp.where(sub // 4 == 0, q, south)
            spin = 2.0 * cos_sin((2 * lats + 1).astype(F32), plan.lat * 1.0, plan.lat * 4.0)[0]
            angles = table[first : first + points, :]
            sides = lax.dot_general(coefs[at], angles, NT, preferred_element_type=F32)
            even, odd, even2, odd2 = (sides[32 * i : 32 * i + 32] for i in range(4))
            point = iota((1, points), 1).astype(F32)
            below_end = point < quart
            up_to_end = point <= quart
            later = point > 0.0
            products = []
            for grid, inside in (
                (even - odd, up_to_end),
                (even + odd, up_to_end & later),
                (even2 - odd2, below_end),
                (even2 + odd2, below_end & later),
            ):
                u, v, vort, temp = grid[0:8], grid[8:16], grid[16:24], grid[24:32]
                absolute = vort + spin
                for p in (absolute * u, absolute * v, 0.5 * (u * u + v * v), u * temp):
                    products.append(jnp.where(inside, p, 0.0))
            products = jnp.concatenate(products, axis=0).astype(BF16)
            back = jnp.dot(products, angles, preferred_element_type=F32)
            b1, b2, b3, b4 = (back[32 * i : 32 * i + 32] for i in range(4))
            real = (b1 + b2)[:, 0:128] + parity * (b3 + b4)[:, 0:128]
            imag = (b2 - b1)[:, 128:256] + parity * (b3 - b4)[:, 128:256]
            is_south = iota((32, 1), 0) // 4 % 2 == 1
            scale = jnp.where(is_south, quad[south], quad[q]) / length
            sums.append((jnp.where(keep[at], real * scale, 0.0), jnp.where(keep[at], imag * scale, 0.0)))
        merged = jnp.concatenate([sums[0][0], sums[1][0], sums[0][1], sums[1][1]], axis=0).T
        for slot in range(2):
            stage[pl.ds(slot * quads + b, n, stride=rows), :] = merged[slot * n : (slot + 1) * n]
    ret_out[...] = stage[...].astype(BF16)

    def send_back(to):
        pltpu.make_async_remote_copy(
            message(ret_out, to), message(ret_in, me), ret_send, ret_recv, device_id={"wave": to}, device_id_type=MESH
        ).start()

    partners(send_back)
    pltpu.make_async_copy(message(ret_out, me), message(ret_in, me), ret_recv).start()

    def wait_level(k, acc):
        level_copy(k, lev).wait_recv()
        return acc + level_in[k]

    deeper = lax.fori_loop(lev + 1, depth, wait_level, jnp.zeros((4, span), F32))
    for slot in range(2):
        for part in range(2):
            at = slot * 2 + part
            below[slot, part] = below[slot, part] + deeper[at : at + 1]
    row_of = iota((128, 128), 0)
    picked_of = (row_of // 16 % 2) * 64 + (row_of // 4 % 4) * 8 + row_of % 4
    picked_of = picked_of + which_of(row_of // 32) * 32 + (row_of // 64) * 4
    pick = (iota((128, 128), 1) == picked_of).astype(BF16)

    pltpu.make_async_copy(ret_in, ret_in, ret_recv).wait()
    stage[...] = ret_in[...].astype(F32)
    for slot in range(2):
        rows_in = [stage[pl.ds(slot * quads + b, n, stride=rows), :] for b in range(quads)]
        rows_in = jnp.concatenate(rows_in, axis=0).astype(BF16)
        left = lax.dot_general(pick, rows_in, NT, preferred_element_type=F32).astype(BF16)
        zero = jnp.zeros((4, span), F32)
        acc = jnp.concatenate([zero, zero, below[slot, 0], zero, zero, zero, below[slot, 1], zero], axis=0)
        for k in range(4):
            acc = acc + jnp.dot(left[k * 32 : k * 32 + 32], block(slot, k), preferred_element_type=F32)
        live = column < span - waves[slot]
        out_ref[slot] = jnp.where(live, acc, 0.0).astype(BF16)

    pltpu.make_async_copy(wave_rows.at[others], wave_rows.at[others], wave_send).wait()
    pltpu.make_async_copy(msg_out.at[most], msg_out.at[most], out_send).wait()
    pltpu.make_async_copy(ret_out.at[most], ret_out.at[most], ret_send).wait()

    def sent_level(k, c):
        level_copy(lev, k).wait_send()
        return c

    lax.fori_loop(0, lev, sent_level, 0)


def solution(mesh):
    plan = Plan(mesh)
    n, depth, span, lat = plan.groups, plan.depth, plan.span, plan.lat
    dma = pltpu.SemaphoreType.DMA

    def body(*args):
        any_spec = pl.BlockSpec(memory_space=pltpu.HBM)
        return pl.pallas_call(
            functools.partial(kernel, plan),
            out_shape=jax.ShapeDtypeStruct((2, 32, span), BF16),
            in_specs=[any_spec] * 5,
            out_specs=pl.BlockSpec(memory_space=pltpu.VMEM),
            scratch_shapes=[
                pltpu.VMEM((2, 32, span), BF16),
                pltpu.VMEM((2, lat, span), BF16),
                pltpu.VMEM((2, 2, lat // 4, span), BF16),
                pltpu.SMEM((4,), F32),
                pltpu.SMEM((lat,), F32),
                pltpu.SMEM((2,), jnp.int32),
                pltpu.VMEM((1, 128), F32),
                pltpu.VMEM((n, 128), F32),
                pltpu.VMEM((n * plan.rows, 128), F32),
                pltpu.VMEM((n * plan.rows, 128), BF16),
                pltpu.VMEM((n * plan.rows, 128), BF16),
                pltpu.VMEM((n * plan.rows, 128), BF16),
                pltpu.VMEM((n * plan.rows, 128), BF16),
                pltpu.VMEM((2 * plan.quads, 128, 256), BF16),
                pltpu.VMEM((2 * plan.quads, 2, LOW + plan.coarse, 128), F32),
                pltpu.VMEM((plan.table_rows, 256), BF16),
                pltpu.VMEM((4, span), F32),
                pltpu.VMEM((depth, 4, span), F32),
                pltpu.VMEM((2, 2, 4, span), F32),
                dma((6,)), dma, dma, dma, dma, dma, dma, dma((depth,)), dma((depth,)),
            ],
            compiler_params=pltpu.CompilerParams(
                collective_id=0, has_side_effects=True, vmem_limit_bytes=24 * 1024 * 1024
            ),
        )(*[pltpu.with_memory_space_constraint(x, pltpu.HBM) for x in args])

    in_specs = (P("wave", "lev", None), P("wave", None, None), P("lev"), P(), P("wave"))
    return jax.shard_map(body, mesh=mesh, in_specs=in_specs, out_specs=P("wave", "lev", None), check_vma=False)
```

```python
import functools
import math

import jax
import jax.numpy as jnp
from jax import lax
from jax.experimental import pallas as pl
from jax.experimental.pallas import tpu as pltpu
from jax.sharding import PartitionSpec as P

MESH = pl.DeviceIdType.MESH
F32 = jnp.float32
BF16 = jnp.bfloat16
LOW = 32
AHEAD = 5
NT = (((1,), (1,)), ((), ()))


def round_up(x, step):
    return -(-x // step) * step


def iota(shape, dim):
    return lax.broadcasted_iota(jnp.int32, shape, dim)


def cos_sin(turns, quarter, length):
    count = jnp.floor(turns * (1.0 / quarter) + 0.5)
    x = (turns - count * quarter) * (2.0 * math.pi / length)
    y = x * x
    sine = x + x * y * (-1 / 6 + y * (1 / 120 + y * (-1 / 5040 + y * (1 / 362880))))
    cosine = 1.0 + y * (-0.5 + y * (1 / 24 + y * (-1 / 720 + y * (1 / 40320))))
    turn = count.astype(jnp.int32)
    swap = (turn & 1) == 1
    one = jnp.where(swap, sine, cosine)
    two = jnp.where(swap, cosine, sine)
    return jnp.where(((turn + 1) & 2) == 2, -one, one), jnp.where((turn & 2) == 2, -two, two)


class Plan:
    def __init__(self, mesh):
        self.groups = mesh.shape["wave"]
        self.depth = mesh.shape["lev"]
        self.lat = 1280
        self.span = 640
        self.quarter = self.lat // 4
        self.quads = self.quarter // self.groups
        self.rows = 2 * self.quads
        self.blocks = []
        first = 0
        for quad in range(self.quads):
            low = quad * self.groups
            high = low + self.groups - 1
            for which in range(2):
                longest = 6 + (high if which == 0 else self.lat // 2 - 1 - low)
                points = round_up(longest, 128)
                self.blocks.append((quad, which, points, first))
                first += points
        self.table_rows = first
        self.coarse = round_up(max(b[2] for b in self.blocks), 8 * LOW) // LOW


def kernel(
    plan,
    spec_hbm, leg_hbm, share_hbm, quad_hbm, wave_hbm, out_ref,
    spec, leg, leg_turned, share, quad, waves,
    wave_row, wave_rows, wave_all, stage, stage_out, msg_out, msg_in, ret_out, ret_in,
    coefs, base, table, level_out, level_in, below,
    load_sem, wave_send, wave_recv, pass_send, pass_recv, out_send, out_recv, ret_send, ret_recv, lev_send, lev_recv,
):
    n, depth, quads, span = plan.groups, plan.depth, plan.quads, plan.span
    me = lax.axis_index("wave")
    lev = lax.axis_index("lev")
    quarter, rows = plan.quarter, plan.rows

    def partners(visit):
        def at(offset):
            to = me + offset
            visit(jnp.where(to >= n, to - n, to))

        def both(p):
            at(n // 2 - p)
            at(n // 2 + p)

        def several(i, c):
            for u in range(3):
                both(3 * i + u + 1)
            return c

        at(n // 2)
        lax.fori_loop(0, (n // 2 - 1) // 3, several, 0)
        for p in range((n // 2 - 1) // 3 * 3 + 1, n // 2):
            both(p)

    def message(ref, k):
        return ref.at[pl.ds(pl.multiple_of(k * rows, 2), rows)]

    loads = [
        pltpu.make_async_copy(wave_hbm, waves, load_sem.at[0]),
        pltpu.make_async_copy(spec_hbm, spec, load_sem.at[1]),
        pltpu.make_async_copy(share_hbm, share, load_sem.at[2]),
        pltpu.make_async_copy(quad_hbm, quad, load_sem.at[3]),
        pltpu.make_async_copy(leg_hbm.at[0], leg.at[0], load_sem.at[4]),
        pltpu.make_async_copy(leg_hbm.at[1], leg.at[1], load_sem.at[5]),
    ]
    for load in loads:
        load.start()

    barrier = pltpu.get_barrier_semaphore()

    def greet(to):
        pl.semaphore_signal(barrier, inc=1, device_id={"wave": to}, device_id_type=MESH)

    partners(greet)

    def greet_level(k, c):
        pl.semaphore_signal(barrier, inc=1, device_id={"lev": k}, device_id_type=MESH)
        return c

    lax.fori_loop(lev + 1, depth, greet_level, 0)

    loads[0].wait()
    lane = iota((1, 128), 1)
    row = jnp.where(lane == me, waves[0], 0) + jnp.where(lane == me + n, waves[1], 0)
    wave_row[...] = row.astype(F32)
    loads[1].wait()
    loads[2].wait()

    column = iota((1, span), 1)
    masked = []
    for slot in range(2):
        live = column < span - waves[slot]
        values = jnp.where(live, spec[slot].astype(F32), 0.0)
        masked.append(values.astype(BF16))
        for part in range(2):
            total = jnp.zeros((1, span), F32)
            for l in (3, 2, 1, 0):
                at = part * 16 + 12 + l
                total = total + values[at : at + 1] * share[l]
                below[slot, part, l : l + 1, :] = total
            level_out[slot * 2 + part : slot * 2 + part + 1, :] = total

    def which_of(k):
        return (k + 1) // 2 % 2

    where_row, where_col = iota((128, 32), 0), iota((128, 32), 1)
    column_of = (where_col // 16) * 64 + (where_col // 4 % 4) * 8 + where_col % 4
    place = [(where_row == column_of + which_of(k) * 32 + (k // 2) * 4).astype(BF16) for k in range(4)]
    flip = (iota((n, n), 0) + iota((n, n), 1) == n - 1).astype(BF16)

    def block(slot, k):
        if k % 2:
            return leg_turned[slot, k // 2]
        return leg[slot, k * quarter : (k + 1) * quarter, :]

    for slot in range(2):
        loads[4 + slot].wait()
        for k in (1, 3):
            for b in range(quads):
                old = k * quarter + (quads - 1 - b) * n
                turned = jnp.dot(flip, leg[slot, old : old + n, :], preferred_element_type=F32)
                leg_turned[slot, k // 2, b * n : (b + 1) * n, :] = turned.astype(BF16)
        acc = None
        for k in range(4):
            weights = jnp.dot(place[k], masked[slot], preferred_element_type=F32).astype(BF16)
            term = lax.dot_general(block(slot, k), weights, NT, preferred_element_type=F32)
            acc = term if acc is None else acc + term
        for b in range(quads):
            stage[pl.ds(slot * quads + b, n, stride=rows), :] = acc[b * n : (b + 1) * n]
    msg_out[...] = stage[...].astype(BF16)

    pl.semaphore_wait(barrier, n - 1 + lev)

    def send_wave(to):
        pltpu.make_async_remote_copy(
            wave_row, wave_rows.at[pl.ds(me, 1)], wave_send, wave_recv, device_id={"wave": to}, device_id_type=MESH
        ).start()

    @pl.when(lev > 0)
    def _():
        partners(send_wave)
        pltpu.make_async_copy(wave_row, wave_rows.at[pl.ds(me, 1)], wave_recv).start()

    def send_out(to):
        pltpu.make_async_remote_copy(
            message(msg_out, to), message(msg_in, me), out_send, out_recv, device_id={"wave": to}, device_id_type=MESH
        ).start()

    partners(send_out)

    def level_copy(source, to):
        return pltpu.make_async_remote_copy(
            level_out, level_in.at[source], lev_send.at[to], lev_recv.at[source],
            device_id={"lev": to}, device_id_type=MESH,
        )

    def send_level(k, c):
        level_copy(lev, k).start()
        return c

    lax.fori_loop(0, lev, send_level, 0)
    pltpu.make_async_copy(message(msg_out, me), message(msg_in, me), out_recv).start()
    others, most = pl.ds(0, n - 1), pl.ds(0, (n - 1) * rows)
    loads[3].wait()

    pass_on = pltpu.make_async_remote_copy(
        wave_all, wave_all, pass_send, pass_recv, device_id={"lev": 0}, device_id_type=MESH
    )

    @pl.when(lev > 0)
    def _():
        pltpu.make_async_copy(wave_rows, wave_rows, wave_recv).wait()
        wave_all[...] = jnp.sum(wave_rows[...], axis=0, keepdims=True)

    @pl.when(lev == 1)
    def _():
        pass_on.start()

    @pl.when(lev == 0)
    def _():
        pass_on.wait_recv()

    m = wave_all[...]

    index = iota((24, 1), 0)
    step = jnp.where(index < 8, index, jnp.where(index < 12, (index - 8) * 8, (index - 12) * 256))
    step = jnp.where(index < 16, step, (index - 16) * LOW).astype(F32)
    turns = step * m
    lengths = {}
    keep = {}
    double = jnp.where(m == 0.0, 1.0, 2.0)
    parity = 1.0 - 2.0 * (m - 2.0 * jnp.floor(m * 0.5))

    def rotated(c, s, at, r):
        ch, sh = base[at, 0, r : r + 1, :], base[at, 1, r : r + 1, :]
        return ch * c - sh * s, sh * c + ch * s

    def make_tables(b):
        for which in range(2):
            at = 2 * b + which
            _, _, points, first = plan.blocks[at]
            q = me + b * n
            if which == 1:
                q = plan.lat // 2 - 1 - q
            quart = (5 + q).astype(F32)
            lengths[at] = (q, quart, quart * 4.0)
            keep[at] = 2.0 * m < quart * 4.0
            c, s = cos_sin(turns, quart, quart * 4.0)
            base[at, 0, 0:24], base[at, 1, 0:24] = c, s
            fine = [(c[0:8], s[0:8])] + [rotated(c[0:8], s[0:8], at, 8 + r) for r in range(1, 4)]
            cl = jnp.concatenate([f[0] for f in fine], axis=0)
            sl = jnp.concatenate([f[1] for f in fine], axis=0)
            for r in range(1, round_up(points, 256) // 256):
                high = rotated(c[16:24], s[16:24], at, 12 + r)
                base[at, 0, 16 + 8 * r : 24 + 8 * r], base[at, 1, 16 + 8 * r : 24 + 8 * r] = high
            for a in range(points // LOW):
                to = first + a * LOW
                ct, st = rotated(cl, sl, at, 16 + a)
                table[to : to + LOW, 0:128] = ct.astype(BF16)
                table[to : to + LOW, 128:256] = st.astype(BF16)

    none = jnp.zeros((32, 128), F32)

    def make_coefs(b):
        rows_in = [stage[pl.ds(slot * quads + b, n, stride=rows), :] for slot in range(2)]
        turned = jnp.concatenate(rows_in, axis=0).T
        for which in range(2):
            amplitude = jnp.where(keep[2 * b + which], double, 0.0)
            real = turned[which * 32 : which * 32 + 32] * amplitude
            imag = turned[64 + which * 32 : 96 + which * 32] * amplitude
            left = jnp.concatenate([real, none, real * parity, none], axis=0)
            right = jnp.concatenate([none, imag, none, imag * -parity], axis=0)
            coefs[2 * b + which] = jnp.concatenate([left, right], axis=1).astype(BF16)

    for b in range(AHEAD):
        make_tables(b)
    pltpu.make_async_copy(msg_in, msg_in, out_recv).wait()
    stage[...] = msg_in[...].astype(F32)
    for b in range(AHEAD):
        make_coefs(b)

    sub = iota((8, 1), 0)
    for b in range(quads):
        if b + AHEAD < quads:
            make_tables(b + AHEAD)
            make_coefs(b + AHEAD)
        sums = []
        for which in range(2):
            at = 2 * b + which
            _, _, points, first = plan.blocks[at]
            q, quart, length = lengths[at]
            south = plan.lat - 1 - q
            lats = jnp.where(sub // 4 == 0, q, south)
            spin = 2.0 * cos_sin((2 * lats + 1).astype(F32), plan.lat * 1.0, plan.lat * 4.0)[0]
            angles = table[first : first + points, :]
            sides = lax.dot_general(coefs[at], angles, NT, preferred_element_type=F32)
            even, odd, even2, odd2 = (sides[32 * i : 32 * i + 32] for i in range(4))
            point = iota((1, points), 1).astype(F32)
            below_end = point < quart
            up_to_end = point <= quart
            later = point > 0.0
            products = []
            for grid, inside in (
                (even - odd, up_to_end),
                (even + odd, up_to_end & later),
                (even2 - odd2, below_end),
                (even2 + odd2, below_end & later),
            ):
                u, v, vort, temp = grid[0:8], grid[8:16], grid[16:24], grid[24:32]
                absolute = vort + spin
                for p in (absolute * u, absolute * v, 0.5 * (u * u + v * v), u * temp):
                    products.append(jnp.where(inside, p, 0.0))
            products = jnp.concatenate(products, axis=0).astype(BF16)
            back = jnp.dot(products, angles, preferred_element_type=F32)
            b1, b2, b3, b4 = (back[32 * i : 32 * i + 32] for i in range(4))
            real = (b1 + b2)[:, 0:128] + parity * (b3 + b4)[:, 0:128]
            imag = (b2 - b1)[:, 128:256] + parity * (b3 - b4)[:, 128:256]
            is_south = iota((32, 1), 0) // 4 % 2 == 1
            scale = jnp.where(is_south, quad[south], quad[q]) / length
            sums.append((jnp.where(keep[at], real * scale, 0.0), jnp.where(keep[at], imag * scale, 0.0)))
        merged = jnp.concatenate([sums[0][0], sums[1][0], sums[0][1], sums[1][1]], axis=0).T
        for slot in range(2):
            stage_out[pl.ds(slot * quads + b, n, stride=rows), :] = merged[slot * n : (slot + 1) * n]
    ret_out[...] = stage_out[...].astype(BF16)

    def send_back(to):
        pltpu.make_async_remote_copy(
            message(ret_out, to), message(ret_in, me), ret_send, ret_recv, device_id={"wave": to}, device_id_type=MESH
        ).start()

    partners(send_back)
    pltpu.make_async_copy(message(ret_out, me), message(ret_in, me), ret_recv).start()

    def wait_level(k, acc):
        level_copy(k, lev).wait_recv()
        return acc + level_in[k]

    deeper = lax.fori_loop(lev + 1, depth, wait_level, jnp.zeros((4, span), F32))
    for slot in range(2):
        for part in range(2):
            at = slot * 2 + part
            below[slot, part] = below[slot, part] + deeper[at : at + 1]
    row_of = iota((128, 128), 0)
    picked_of = (row_of // 16 % 2) * 64 + (row_of // 4 % 4) * 8 + row_of % 4
    picked_of = picked_of + which_of(row_of // 32) * 32 + (row_of // 64) * 4
    pick = (iota((128, 128), 1) == picked_of).astype(BF16)

    pltpu.make_async_copy(ret_in, ret_in, ret_recv).wait()
    stage[...] = ret_in[...].astype(F32)
    for slot in range(2):
        rows_in = [stage[pl.ds(slot * quads + b, n, stride=rows), :] for b in range(quads)]
        rows_in = jnp.concatenate(rows_in, axis=0).astype(BF16)
        left = lax.dot_general(pick, rows_in, NT, preferred_element_type=F32).astype(BF16)
        zero = jnp.zeros((4, span), F32)
        acc = jnp.concatenate([zero, zero, below[slot, 0], zero, zero, zero, below[slot, 1], zero], axis=0)
        for k in range(4):
            acc = acc + jnp.dot(left[k * 32 : k * 32 + 32], block(slot, k), preferred_element_type=F32)
        live = column < span - waves[slot]
        out_ref[slot] = jnp.where(live, acc, 0.0).astype(BF16)

    @pl.when(lev > 0)
    def _():
        pltpu.make_async_copy(wave_rows.at[others], wave_rows.at[others], wave_send).wait()

    @pl.when(lev == 1)
    def _():
        pass_on.wait_send()

    pltpu.make_async_copy(msg_out.at[most], msg_out.at[most], out_send).wait()
    pltpu.make_async_copy(ret_out.at[most], ret_out.at[most], ret_send).wait()

    def sent_level(k, c):
        level_copy(lev, k).wait_send()
        return c

    lax.fori_loop(0, lev, sent_level, 0)


def solution(mesh):
    plan = Plan(mesh)
    n, depth, span, lat = plan.groups, plan.depth, plan.span, plan.lat
    dma = pltpu.SemaphoreType.DMA

    def body(*args):
        any_spec = pl.BlockSpec(memory_space=pltpu.HBM)
        return pl.pallas_call(
            functools.partial(kernel, plan),
            out_shape=jax.ShapeDtypeStruct((2, 32, span), BF16),
            in_specs=[any_spec] * 5,
            out_specs=pl.BlockSpec(memory_space=pltpu.VMEM),
            scratch_shapes=[
                pltpu.VMEM((2, 32, span), BF16),
                pltpu.VMEM((2, lat, span), BF16),
                pltpu.VMEM((2, 2, lat // 4, span), BF16),
                pltpu.SMEM((4,), F32),
                pltpu.SMEM((lat,), F32),
                pltpu.SMEM((2,), jnp.int32),
                pltpu.VMEM((1, 128), F32),
                pltpu.VMEM((n, 128), F32),
                pltpu.VMEM((1, 128), F32),
                pltpu.VMEM((n * plan.rows, 128), F32),
                pltpu.VMEM((n * plan.rows, 128), F32),
                pltpu.VMEM((n * plan.rows, 128), BF16),
                pltpu.VMEM((n * plan.rows, 128), BF16),
                pltpu.VMEM((n * plan.rows, 128), BF16),
                pltpu.VMEM((n * plan.rows, 128), BF16),
                pltpu.VMEM((2 * plan.quads, 128, 256), BF16),
                pltpu.VMEM((2 * plan.quads, 2, 16 + plan.coarse, 128), F32),
                pltpu.VMEM((plan.table_rows, 256), BF16),
                pltpu.VMEM((4, span), F32),
                pltpu.VMEM((depth, 4, span), F32),
                pltpu.VMEM((2, 2, 4, span), F32),
                dma((6,)), dma, dma, dma, dma, dma, dma, dma, dma, dma((depth,)), dma((depth,)),
            ],
            compiler_params=pltpu.CompilerParams(
                collective_id=0, has_side_effects=True, vmem_limit_bytes=24 * 1024 * 1024
            ),
        )(*[pltpu.with_memory_space_constraint(x, pltpu.HBM) for x in args])

    in_specs = (P("wave", "lev", None), P("wave", None, None), P("lev"), P(), P("wave"))
    return jax.shard_map(body, mesh=mesh, in_specs=in_specs, out_specs=P("wave", "lev", None), check_vma=False)
```
